32 devices in a mesh: groups: 2 (over x), section: 8 (over z, y), head: 2 (over core).
Axes of the slice: x: 2, y: 2, z: 4, core: 2. Of those that a mesh axis runs over, the one named last changes fastest.
Arguments:
- video_tokens: bfloat16 [8192, 1536], P(('groups', 'section', 'head')), parts along dimension 0, may hold values from -6 to 6
- modulation: float32 [6, 1536], P('groups'), parts along dimension 0, may hold values from -3 to 3
- project_weight: bfloat16 [3, 1536, 1536], P(None, None, 'head'), may hold values from -0.15625 to 0.15625
- output_weight: bfloat16 [1536, 1536], P('head'), may hold values from -0.15625 to 0.15625
- norm_gains: float32 [3, 128], replicated, may hold values from 1 to 2
- text_cache: bfloat16 [2, 512, 1536], P(None, 'groups', 'head'), parts along dimension 1, may hold values from -6 to 6
- text_count: int32 [2], P('groups'), parts along dimension 0, may hold values from 1 to 256, as said below
- video_keep: int32 [8192], P('groups'), parts along dimension 0, may hold values 0 or 1
- patch_order: int32 [16], P('groups'), parts along dimension 0, may hold values from 0 to 7, each once
- stale_cache: bfloat16 [2, 8192, 1536], P(None, ('groups', 'section'), 'head'), parts along dimension 1, may hold values from -6 to 6
Outputs:
- updated: bfloat16 [8192, 1536], P(('groups', 'section', 'head')), parts along dimension 0
- fresh_cache: bfloat16 [2, 8192, 1536], P(None, ('groups', 'section'), 'head'), parts along dimension 1
The draws below stay inside these ranges and needn't reach their ends.
There are 2 independent parts, one for each index of `groups`. The reference program is written for one: setup_inputs(seed, part) draws one part's arguments, and reference() takes and returns one part's arrays. A program takes and returns all parts, laid end to end along the dimension named above; an argument that names none is the same for every part. Nothing has to cross between parts.
Inputs may be any that keep to these rules, and one draw needn't show every extreme that they name: The first text_count text tokens are real, the rest are padding. `video_keep`: 1 keeps a video token as a key, 0 marks padding. `patch_order`: each place 0 to 7 is held by exactly one patch.
All inputs are finite; a program needn't handle non-finite values.
Results may differ from the reference program's by a relative error of at most 0.0049.
Values may be sent and summed in bfloat16 or wider, within the bound.
A program may use at most 128 MiB of HBM per device.

```python
import jax
import jax.numpy as jnp
from jax import lax

D = 1536
HEADS = 12
HEAD_DIM = 128
TEXT = 256
PATCH = 512
HID = 1536
SEQ = 4096
N_SECTION = 8


def draw_text_count(key, part):
    short = jax.random.randint(key, (1,), 1, TEXT // 2 + 1, dtype=jnp.int32)
    odd_part = jnp.asarray(part, jnp.int32) % 2 == 1
    return jnp.where(odd_part, jnp.full((1,), TEXT, jnp.int32), short).astype(jnp.int32)


def with_ends(entries, key, low, top_value):
    extent = entries.shape
    place = [jax.random.randint(jax.random.fold_in(key, axis), (), 0, extent[axis]) for axis in range(len(extent))]
    entries = entries.at[tuple(place)].set(low)
    longest = extent.index(max(extent))
    place[longest] = (place[longest] + 1) % extent[longest]
    return entries.at[tuple(place)].set(top_value)


def block_levels(own_key, dims, cuts, least, largest):
    loudness = 1.0
    for position, blocks in cuts:
        steps = jax.random.uniform(jax.random.fold_in(jax.random.fold_in(own_key, 6), position), (blocks,), jnp.float32, least / len(cuts), largest / len(cuts))
        loudness = loudness * jnp.repeat(jnp.exp(steps), dims[position] // blocks).reshape((-1,) + (1,) * (len(dims) - 1 - position))
    return loudness


def normal_values(rng, dims, deviation, most, split=(), kind=jnp.bfloat16):
    result = deviation * jax.random.normal(rng, dims, jnp.float32)
    if split:
        result = result * block_levels(rng, dims, split, -0.22, 0.18)
    return jnp.clip(result, -most, most).astype(kind)


def setup_inputs(seed: int = 0, part: int = 0) -> dict:
    streams_of = jax.random.split(jax.random.key(seed), 11)
    own_keys = jax.random.split(jax.random.fold_in(streams_of[10], part), 11)
    video_tokens = normal_values(own_keys[0], (SEQ, D), 1.0, 6.0, ((0, 16),))
    modulation = normal_values(own_keys[1], (3, D), 0.7, 3.0, (), jnp.float32)
    project_weight = normal_values(streams_of[2], (3, D, HID), D ** -0.5, 0.15625, ((2, 2),))
    output_weight = normal_values(streams_of[3], (HID, D), HID ** -0.5, 0.15625, ((0, 2),))
    norm_gains = jnp.clip(jax.random.uniform(streams_of[4], (3, HEAD_DIM), jnp.float32, 1.0, 2.0), 1.0, 2.0)
    text_cache = normal_values(own_keys[5], (2, TEXT, HID), 1.4, 6.0, ((2, 2),))
    text_count = draw_text_count(jax.random.fold_in(jax.random.fold_in(streams_of[10], part), 71), part)
    video_keep = with_ends((jax.random.randint(own_keys[7], (SEQ,), 0, 4) < 3).astype(jnp.int32), jax.random.fold_in(own_keys[7], 1), 0, 1)
    patch_order = jax.random.permutation(own_keys[8], N_SECTION).astype(jnp.int32)
    stale_cache = normal_values(own_keys[9], (2, SEQ, HID), 1.4, 6.0, ((1, 8), (2, 2)))
    return dict(video_tokens=video_tokens, modulation=modulation, project_weight=project_weight, output_weight=output_weight, norm_gains=norm_gains, text_cache=text_cache, text_count=text_count, video_keep=video_keep, patch_order=patch_order, stale_cache=stale_cache)


epsilon = 1e-06

def widen(array):
    return lax.optimization_barrier(array).astype(jnp.float32)

def layer_norm(values):
    center = lax.optimization_barrier(jnp.mean(values, axis=-1, keepdims=True))
    shifted = values - center
    spread = lax.optimization_barrier(jnp.mean(shifted * shifted, axis=-1, keepdims=True))
    return shifted * lax.rsqrt(spread + epsilon)

def head_norm(inputs, gain_row):
    per_head = inputs.reshape(inputs.shape[0], HEADS, HEAD_DIM)
    scaled = per_head * lax.rsqrt(lax.optimization_barrier(jnp.mean(per_head * per_head, axis=-1, keepdims=True)) + epsilon) * gain_row
    return scaled.astype(jnp.bfloat16)

def reference(video_tokens, modulation, project_weight, output_weight, norm_gains, text_cache, text_count, video_keep, patch_order, stale_cache):
    hidden = video_tokens.astype(jnp.float32)
    normed = (layer_norm(hidden) * (1.0 + modulation[1]) + modulation[0]).astype(jnp.bfloat16)
    projected = jnp.einsum('sd,cdh->csh', widen(normed), project_weight.astype(jnp.float32), precision=lax.Precision.HIGHEST)
    fresh_cache = projected[1:3].astype(jnp.bfloat16)
    queries = head_norm(projected[0], norm_gains[0])
    fresh_keys = head_norm(widen(fresh_cache[0]), norm_gains[1])
    stale_keys = head_norm(stale_cache[0].astype(jnp.float32), norm_gains[1])
    text_keys = head_norm(text_cache[0].astype(jnp.float32), norm_gains[2])
    fresh_values = fresh_cache[1].reshape(SEQ, HEADS, HEAD_DIM)
    stale_values = stale_cache[1].reshape(SEQ, HEADS, HEAD_DIM)
    text_values = text_cache[1].reshape(TEXT, HEADS, HEAD_DIM)
    text_live = jnp.arange(TEXT, dtype=jnp.int32) < text_count[0]
    score_scale = HEAD_DIM ** (-0.5)

    def rows_of(array, patch_index):
        return lax.dynamic_slice_in_dim(array, (patch_index * PATCH).astype(jnp.int32), PATCH, 0)

    def one_patch(patch_index):
        left_place = jnp.maximum(patch_index - 1, 0).astype(jnp.int32)
        right_place = jnp.minimum(patch_index + 1, N_SECTION - 1).astype(jnp.int32)
        own_slot = patch_order[patch_index]
        left_fresh = patch_order[left_place] < own_slot
        right_fresh = patch_order[right_place] < own_slot
        left_keys = jnp.where(left_fresh, rows_of(fresh_keys, left_place), rows_of(stale_keys, left_place))
        right_keys = jnp.where(right_fresh, rows_of(fresh_keys, right_place), rows_of(stale_keys, right_place))
        left_values = jnp.where(left_fresh, rows_of(fresh_values, left_place), rows_of(stale_values, left_place))
        right_values = jnp.where(right_fresh, rows_of(fresh_values, right_place), rows_of(stale_values, right_place))
        key_rows = jnp.concatenate([left_keys, rows_of(fresh_keys, patch_index), right_keys, text_keys], axis=0)
        value_rows = jnp.concatenate([left_values, rows_of(fresh_values, patch_index), right_values, text_values], axis=0)
        key_live = jnp.concatenate([(rows_of(video_keep, left_place) > 0) & (patch_index > 0), rows_of(video_keep, patch_index) > 0, (rows_of(video_keep, right_place) > 0) & (patch_index < N_SECTION - 1), text_live])
        query_rows = rows_of(queries, patch_index)
        scores = jnp.einsum('qhd,khd->hqk', query_rows.astype(jnp.float32), key_rows.astype(jnp.float32), precision=lax.Precision.HIGHEST) * score_scale
        weights = jnp.where(key_live[None, None, :], jnp.exp(scores), 0.0)
        total = lax.optimization_barrier(jnp.sum(weights, axis=-1))
        numerator = jnp.einsum('hqk,khd->qhd', widen(weights.astype(jnp.bfloat16)), value_rows.astype(jnp.float32), precision=lax.Precision.HIGHEST)
        return (numerator / jnp.transpose(total)[:, :, None]).astype(jnp.bfloat16).reshape(PATCH, HID)
    attended = lax.map(one_patch, jnp.arange(N_SECTION, dtype=jnp.int32)).reshape(SEQ, HID)
    mixed = jnp.dot(attended, output_weight, preferred_element_type=jnp.float32)
    updated = (hidden + modulation[2] * mixed).astype(jnp.bfloat16)
    return (updated, fresh_cache)
```

```python
import jax
import jax.numpy as jnp
from jax import lax
from jax.experimental import pallas as pl
from jax.experimental.pallas import tpu as pltpu
from jax.sharding import PartitionSpec as P

epsilon = 1e-06
log2_e = 1.4426950408889634
MESH = pl.DeviceIdType.MESH
f32 = jnp.float32
bf16 = jnp.bfloat16


def dot_nt(a, b):
    return lax.dot_general(a, b, (((1,), (1,)), ((), ())), preferred_element_type=f32)


def head_norm(rows, gain):
    return rows * lax.rsqrt(jnp.mean(rows * rows, axis=-1, keepdims=True) + epsilon) * gain


def kernel(
    order_hbm,
    count_hbm,
    tokens_hbm,
    modulation_hbm,
    gains_hbm,
    keep_hbm,
    weight_hbm,
    output_weight_hbm,
    text_hbm,
    stale_hbm,
    base,
    last,
    last_weight,
    modulation_ref,
    raw,
    order_ref,
    count_ref,
    tokens_ref,
    gains_ref,
    keep_ref,
    weight,
    output_weight,
    text,
    stale,
    normed,
    query,
    query_mate,
    query_far,
    keys,
    values,
    text_keys,
    text_values,
    own_sum,
    mate_sum,
    far_out,
    far_total_out,
    far_in,
    far_total_in,
    back_out,
    back_total_out,
    back_in,
    back_total_in,
    attended,
    mixed_out,
    mixed_in,
    load_sem,
    normed_sem,
    query_sem,
    forward_sem,
    far_sem,
    far_total_sem,
    back_sem,
    back_total_sem,
    mixed_sem,
):
    count = lax.axis_size("section")
    me = lax.axis_index("section")
    core = lax.axis_index("head")
    other_core = 1 - core
    parity = lax.rem(me, 2)
    mate = me + 1 - 2 * parity
    step = 2 - 4 * parity
    ahead = me + step
    behind = me - step
    has_ahead = jnp.logical_and(ahead >= 0, ahead < count)
    has_behind = jnp.logical_and(behind >= 0, behind < count)
    rows = tokens_hbm.shape[0]
    head = gains_ref.shape[1]
    width = weight.shape[2]
    heads = width // head
    units = 2 * heads
    patch = 2 * rows

    factor = head ** (-0.5) * log2_e
    pair = 2 if heads % 2 == 0 else 1
    span = pair * head
    pairs = heads // pair
    early = min(3, heads)

    def columns(step_index):
        return pl.ds(pl.multiple_of(step_index * span, span), span)

    def load(place, source, target):
        return pltpu.make_async_copy(source, target, load_sem.at[place])

    small = [
        load(place, source, target)
        for place, (source, target) in enumerate(
            (
                (tokens_hbm, tokens_ref),
                (modulation_hbm, modulation_ref),
                (gains_hbm, gains_ref),
            )
        )
    ]
    query_weights = [
        load(3 + c, weight_hbm.at[0, :, columns(c)], weight.at[0, :, columns(c)])
        for c in range(pairs)
    ]
    place = 3 + pairs
    key_weights = load(place, weight_hbm.at[1], weight.at[1])
    value_weights = load(place + 1, weight_hbm.at[2], weight.at[2])
    stale_load = load(place + 2, stale_hbm, stale)
    text_load = load(place + 3, text_hbm, text)
    keep_load = load(place + 4, keep_hbm, keep_ref)
    order_load = load(place + 5, order_hbm, order_ref)
    count_load = load(place + 6, count_hbm, count_ref)
    turned = width - span
    output_loads = [
        load(place + 7, output_weight_hbm.at[turned:width], output_weight.at[0:span]),
        load(place + 9, output_weight_hbm.at[turned - head : turned], last_weight),
    ]
    if turned > 0:
        output_loads.append(
            load(place + 8, output_weight_hbm.at[0:turned], output_weight.at[span:width])
        )
    for copy in small:
        copy.start()
    for c in range(pairs):
        query_weights[pairs - 1 - c].start()

    barrier = pltpu.get_barrier_semaphore()
    pl.semaphore_signal(barrier, inc=1, device_id={"head": other_core}, device_id_type=MESH)
    pl.semaphore_signal(barrier, inc=1, device_id={"section": mate}, device_id_type=MESH)

    @pl.when(has_ahead)
    def _():
        pl.semaphore_signal(barrier, inc=1, device_id={"section": ahead}, device_id_type=MESH)

    @pl.when(has_behind)
    def _():
        pl.semaphore_signal(barrier, inc=1, device_id={"section": behind}, device_id_type=MESH)

    for copy in small:
        copy.wait()
    hidden = tokens_ref[...].astype(f32)
    shifted = hidden - jnp.mean(hidden, axis=-1, keepdims=True)
    spread = jnp.mean(shifted * shifted, axis=-1, keepdims=True)
    normed[0] = (
        shifted * lax.rsqrt(spread + epsilon) * (1.0 + modulation_ref[1:2, :])
        + modulation_ref[0:1, :]
    ).astype(bf16)

    normed_copy = pltpu.make_async_remote_copy(
        src_ref=normed.at[0],
        dst_ref=normed.at[1],
        send_sem=normed_sem.at[0],
        recv_sem=normed_sem.at[1],
        device_id={"head": other_core},
        device_id_type=MESH,
    )

    def remote(source, target, sems, unit, device):
        return pltpu.make_async_remote_copy(
            src_ref=source.at[unit],
            dst_ref=target.at[unit],
            send_sem=sems.at[0, unit],
            recv_sem=sems.at[1, unit],
            device_id={"section": device},
            device_id_type=MESH,
        )

    def query_copy(unit):
        return remote(query, query_mate, query_sem, unit, mate)

    def forward_copy(unit, device):
        return remote(query_mate, query_far, forward_sem, unit, device)

    def far_copies(unit, device):
        return (
            remote(far_out, far_in, far_sem, unit, device),
            remote(far_total_out, far_total_in, far_total_sem, unit, device),
        )

    def back_copies(unit):
        return (
            remote(back_out, back_in, back_sem, unit, mate),
            remote(back_total_out, back_total_in, back_total_sem, unit, mate),
        )

    def project_queries(half, c, first):
        part = jnp.dot(normed[half], weight[0, :, columns(c)], preferred_element_type=f32)
        for j in range(pair):
            query[first + j] = (
                head_norm(part[:, j * head : (j + 1) * head], gains_ref[0:1, :]) * factor
            ).astype(bf16)

    def send_queries(first):
        for j in range(pair):
            query_copy(first + j).start()

    def forward(unit):
        query_copy(unit).wait_recv()

        @pl.when(has_ahead)
        def _():
            forward_copy(unit, ahead).start()

    query_weights[pairs - 1].wait()
    project_queries(0, pairs - 1, 0)

    pl.semaphore_wait(
        barrier, 2 + has_ahead.astype(jnp.int32) + has_behind.astype(jnp.int32)
    )

    normed_copy.start()
    send_queries(0)
    for copy in (key_weights, value_weights, stale_load, text_load, keep_load, order_load, count_load):
        copy.start()
    for copy in output_loads:
        copy.start()
    for c in range(pairs - 1):
        query_weights[c].wait()

    @pl.loop(0, pairs - 1)
    def _(c):
        project_queries(0, c, pair + heads + c * pair)

    normed_copy.wait_recv()

    @pl.loop(0, pairs)
    def _(c):
        project_queries(1, c, pair + c * pair)
        send_queries(pair + c * pair)

    for c in range(pairs - 1):
        send_queries(pair + heads + c * pair)
    key_weights.wait()
    value_weights.wait()
    own_rows = pl.ds(pl.multiple_of(core * rows, rows), rows)
    other_rows = pl.ds(pl.multiple_of(other_core * rows, rows), rows)

    @pl.loop(0, heads // pair)
    def _(c):
        for w in range(2):
            part = jnp.dot(
                normed[...].reshape(patch, normed.shape[2]),
                weight[1 + w, :, columns(c)],
                preferred_element_type=f32,
            ).astype(bf16)
            raw[w, own_rows, columns(c)] = part[0:rows]
            raw[w, other_rows, columns(c)] = part[rows:patch]

        @pl.when(c < early)
        def _():
            forward(c)

    @pl.loop(min(early, heads // pair), early)
    def _(i):
        forward(i)

    for copy in (stale_load, text_load, keep_load, order_load, count_load):
        copy.wait()

    keep_row = keep_ref[pl.ds(pl.multiple_of(me * patch, patch), patch)].astype(f32)
    keep = jnp.transpose(jnp.broadcast_to(keep_row[None, :], (head, patch)))
    text_rows = text.shape[1]
    live = (
        lax.broadcasted_iota(jnp.int32, (text_rows, head), 0) < count_ref[0]
    ).astype(f32)

    @pl.loop(0, heads)
    def _(h):
        lanes = pl.ds(pl.multiple_of(h * head, head), head)
        for version, cache in ((0, raw), (1, stale)):
            keys[version, h] = head_norm(
                cache[0, :, lanes].astype(f32), gains_ref[1:2, :]
            ).astype(bf16)
            values[version, h, :, 0:head] = (cache[1, :, lanes].astype(f32) * keep).astype(bf16)
            values[version, h, :, head : 2 * head] = keep.astype(bf16)
        text_keys[h] = head_norm(text[0, :, lanes].astype(f32), gains_ref[2:3, :]).astype(bf16)
        text_values[h, :, 0:head] = (text[1, :, lanes].astype(f32) * live).astype(bf16)
        text_values[h, :, head : 2 * head] = live.astype(bf16)

    own_slot = order_ref[me]
    mate_version = jnp.where(own_slot < order_ref[mate], 0, 1)
    far_patch = jnp.clip(me - 1 + 2 * parity, 0, count - 1)
    far_version = jnp.where(own_slot < order_ref[far_patch], 0, 1)

    def weighted(queries, key_rows, value_rows):
        weights = jnp.exp2(dot_nt(queries, key_rows)).astype(bf16)
        return jnp.dot(weights, value_rows, preferred_element_type=f32)

    def total_rows(summed):
        return jnp.transpose(summed[:, head : 2 * head])[0:1, :]

    def send_back(unit):
        numerator = mate_sum[unit, :, 0:head]
        totals = total_rows(mate_sum[unit])

        @pl.when(has_ahead)
        def _():
            for copy in far_copies(unit, mate):
                copy.wait_recv()
            back_out[unit] = (numerator + far_in[unit].astype(f32)).astype(bf16)
            back_total_out[unit] = totals + far_total_in[unit]

        @pl.when(jnp.logical_not(has_ahead))
        def _():
            back_out[unit] = numerator.astype(bf16)
            back_total_out[unit] = totals

        for copy in back_copies(unit):
            copy.start()

    @pl.loop(early, units + 2 * early)
    def _(i):
        @pl.when(i < units)
        def _():
            forward(i)

        unit = i - early

        @pl.when(unit < units)
        def _():
            h = lax.rem(unit + heads - pair, heads)

            @pl.when(has_behind)
            def _():
                forward_copy(unit, mate).wait_recv()
                summed = weighted(query_far[unit], keys[far_version, h], values[far_version, h])
                far_out[unit] = summed[:, 0:head].astype(bf16)
                far_total_out[unit] = total_rows(summed)
                for copy in far_copies(unit, behind):
                    copy.start()

            mate_sum[unit] = weighted(
                query_mate[unit], keys[mate_version, h], values[mate_version, h]
            )
            own_sum[unit] = weighted(query[unit], keys[0, h], values[0, h]) + weighted(
                query[unit], text_keys[h], text_values[h]
            )

        @pl.when(i >= 2 * early)
        def _():
            send_back(i - 2 * early)

    def gathered(unit):
        for copy in back_copies(unit):
            copy.wait_recv()
        total = jnp.transpose(jnp.broadcast_to(back_total_in[unit], (head, rows)))
        mine = own_sum[unit]
        return (
            (mine[:, 0:head] + back_in[unit].astype(f32)) / (mine[:, head : 2 * head] + total)
        ).astype(bf16)

    def gather_range(half, first, last_unit, place):
        @pl.loop(first, last_unit)
        def _(unit):
            lanes = pl.ds(pl.multiple_of((unit + place - first) * head, head), head)
            attended[half, :, lanes] = gathered(unit)

    mixed_copy = pltpu.make_async_remote_copy(
        src_ref=mixed_out,
        dst_ref=mixed_in,
        send_sem=mixed_sem.at[0],
        recv_sem=mixed_sem.at[1],
        device_id={"head": other_core},
        device_id_type=MESH,
    )
    full = output_weight.shape[1]
    wide = 512 if full % 512 == 0 else full

    for copy in output_loads:
        copy.wait()
    gather_range(1, pair, pair + heads - pair, pair)
    gather_range(1, heads, pair + heads, 0)

    @pl.loop(0, full // wide)
    def _(c):
        here = pl.ds(pl.multiple_of(c * wide, wide), wide)
        mixed_out[:, here] = jnp.dot(
            attended[1], output_weight[:, here], preferred_element_type=f32
        ).astype(bf16)

    mixed_copy.start()
    gather_range(0, 0, pair, 0)
    gather_range(0, pair + heads, units - 1, pair)
    most = width - head
    mixed_copy.wait_recv()

    @pl.loop(0, full // wide)
    def _(c):
        here = pl.ds(pl.multiple_of(c * wide, wide), wide)
        mixed = mixed_in[:, here].astype(f32) + jnp.dot(
            attended[0, :, 0:most], output_weight[0:most, here], preferred_element_type=f32
        )
        base[:, here] = tokens_ref[:, here].astype(f32) + modulation_ref[2:3, here] * mixed

    last[...] = gathered(units - 1)
    normed_copy.wait_send()
    mixed_copy.wait_send()

    @pl.loop(0, units)
    def _(i):
        query_copy(i).wait_send()
        for copy in back_copies(i):
            copy.wait_send()

        @pl.when(has_ahead)
        def _():
            forward_copy(i, mate).wait_send()

        @pl.when(has_behind)
        def _():
            for copy in far_copies(i, mate):
                copy.wait_send()


def finish(base, last, last_weight, modulation, raw, updated_hbm, raw_hbm, updated, sems):
    full = base.shape[1]
    wide = 512 if full % 512 == 0 else full
    raw_copy = pltpu.make_async_copy(raw, raw_hbm, sems.at[0])
    raw_copy.start()
    copies = []
    for c in range(full // wide):
        here = slice(c * wide, (c + 1) * wide)
        updated[:, here] = (
            base[:, here]
            + modulation[2:3, here]
            * jnp.dot(last[...], last_weight[:, here], preferred_element_type=f32)
        ).astype(bf16)
        copies.append(
            pltpu.make_async_copy(updated.at[:, here], updated_hbm.at[:, here], sems.at[1 + c])
        )
        copies[c].start()
    for copy in copies:
        copy.wait()
    raw_copy.wait()


def on_device(
    video_tokens,
    modulation,
    project_weight,
    output_weight,
    norm_gains,
    text_cache,
    text_count,
    video_keep,
    patch_order,
    stale_cache,
):
    head = norm_gains.shape[1]
    rows, model = video_tokens.shape
    width = project_weight.shape[2]
    patch = stale_cache.shape[1]
    text_rows = text_cache.shape[1]
    heads = width // head
    units = 2 * heads
    pairs = heads // (2 if heads % 2 == 0 else 1)
    vmem = pl.BlockSpec(memory_space=pltpu.VMEM)
    hbm = pl.BlockSpec(memory_space=pl.ANY)
    unit_rows = pltpu.VMEM((units, rows, head), bf16)
    unit_totals = pltpu.VMEM((units, 1, rows), f32)
    unit_sums = pltpu.VMEM((units, rows, 2 * head), f32)
    unit_sems = pltpu.SemaphoreType.DMA((2, units))
    handed = pl.pallas_call(
        kernel,
        out_shape=(
            pltpu.VMEM(video_tokens.shape, f32),
            pltpu.VMEM((rows, head), bf16),
            pltpu.VMEM((head, model), bf16),
            pltpu.VMEM(modulation.shape, f32),
            pltpu.VMEM(stale_cache.shape, bf16),
        ),
        in_specs=[hbm] * 10,
        out_specs=(vmem,) * 5,
        scratch_shapes=[
            pltpu.SMEM(patch_order.shape, jnp.int32),
            pltpu.SMEM(text_count.shape, jnp.int32),
            pltpu.VMEM(video_tokens.shape, bf16),
            pltpu.VMEM(norm_gains.shape, f32),
            pltpu.VMEM(video_keep.shape, jnp.int32),
            pltpu.VMEM(project_weight.shape, bf16),
            pltpu.VMEM(output_weight.shape, bf16),
            pltpu.VMEM(text_cache.shape, bf16),
            pltpu.VMEM(stale_cache.shape, bf16),
            pltpu.VMEM((2, rows, model), bf16),
            unit_rows,
            unit_rows,
            unit_rows,
            pltpu.VMEM((2, heads, patch, head), bf16),
            pltpu.VMEM((2, heads, patch, 2 * head), bf16),
            pltpu.VMEM((heads, text_rows, head), bf16),
            pltpu.VMEM((heads, text_rows, 2 * head), bf16),
            unit_sums,
            unit_sums,
            unit_rows,
            unit_totals,
            unit_rows,
            unit_totals,
            unit_rows,
            unit_totals,
            unit_rows,
            unit_totals,
            pltpu.VMEM((2, rows, width), bf16),
            pltpu.VMEM((rows, model), bf16),
            pltpu.VMEM((rows, model), bf16),
            pltpu.SemaphoreType.DMA((13 + pairs,)),
            pltpu.SemaphoreType.DMA((2,)),
            unit_sems,
            unit_sems,
            unit_sems,
            unit_sems,
            unit_sems,
            unit_sems,
            pltpu.SemaphoreType.DMA((2,)),
        ],
        compiler_params=pltpu.CompilerParams(
            collective_id=0, has_side_effects=True, vmem_limit_bytes=52 * 1024 * 1024
        ),
    )(
        patch_order,
        text_count,
        video_tokens,
        modulation,
        norm_gains,
        video_keep,
        project_weight,
        output_weight,
        text_cache,
        stale_cache,
    )
    return pl.pallas_call(
        finish,
        out_shape=(
            jax.ShapeDtypeStruct(video_tokens.shape, bf16),
            jax.ShapeDtypeStruct(stale_cache.shape, bf16),
        ),
        in_specs=[vmem] * 5,
        out_specs=(hbm, hbm),
        scratch_shapes=[
            pltpu.VMEM(video_tokens.shape, bf16),
            pltpu.SemaphoreType.DMA((1 + model // (512 if model % 512 == 0 else model),)),
        ],
        compiler_params=pltpu.CompilerParams(vmem_limit_bytes=16 * 1024 * 1024),
    )(*[pltpu.with_memory_space_constraint(array, pltpu.VMEM) for array in handed])


def solution(mesh):
    placed = (
        P(("groups", "section", "head"), None),
        P("groups", None),
        P(None, None, "head"),
        P("head", None),
        P(),
        P(None, "groups", "head"),
        P("groups"),
        P("groups"),
        P("groups"),
        P(None, ("groups", "section"), "head"),
    )
    return jax.shard_map(
        on_device,
        mesh=mesh,
        in_specs=placed,
        out_specs=(P(("groups", "section", "head"), None), P(None, ("groups", "section"), "head")),
        check_vma=False,
    )
```

```python
import jax
import jax.numpy as jnp
from jax import lax
from jax.experimental import pallas as pl
from jax.experimental.pallas import tpu as pltpu
from jax.sharding import PartitionSpec as P

epsilon = 1e-06
log2_e = 1.4426950408889634
MESH = pl.DeviceIdType.MESH
f32 = jnp.float32
bf16 = jnp.bfloat16


def dot_nt(a, b):
    return lax.dot_general(a, b, (((1,), (1,)), ((), ())), preferred_element_type=f32)


def head_norm(rows, gain):
    return rows * lax.rsqrt(jnp.mean(rows * rows, axis=-1, keepdims=True) + epsilon) * gain


def kernel(
    order_hbm,
    count_hbm,
    tokens_hbm,
    modulation_hbm,
    gains_hbm,
    keep_hbm,
    weight_hbm,
    output_weight_hbm,
    text_hbm,
    stale_hbm,
    base,
    last,
    last_weight,
    modulation_ref,
    raw,
    order_ref,
    count_ref,
    tokens_ref,
    gains_ref,
    keep_ref,
    weight,
    output_weight,
    text,
    stale,
    normed,
    query,
    query_mate,
    query_far,
    keys,
    values,
    text_keys,
    text_values,
    own_sum,
    mate_sum,
    far_out,
    far_total_out,
    far_in,
    far_total_in,
    back_out,
    back_total_out,
    back_in,
    back_total_in,
    attended,
    mixed_out,
    mixed_in,
    load_sem,
    send_sem,
    normed_sem,
    query_sem,
    forward_sem,
    far_sem,
    far_total_sem,
    back_sem,
    back_total_sem,
    mixed_sem,
    present_sem,
):
    count = lax.axis_size("section")
    me = lax.axis_index("section")
    core = lax.axis_index("head")
    other_core = 1 - core
    parity = lax.rem(me, 2)
    mate = me + 1 - 2 * parity
    step = 2 - 4 * parity
    ahead = me + step
    behind = me - step
    has_ahead = jnp.logical_and(ahead >= 0, ahead < count)
    has_behind = jnp.logical_and(behind >= 0, behind < count)
    barrier = pltpu.get_barrier_semaphore()
    pl.semaphore_signal(barrier, inc=1, device_id={"head": other_core}, device_id_type=MESH)
    pl.semaphore_signal(barrier, inc=1, device_id={"section": mate}, device_id_type=MESH)

    later = me + 2
    earlier = me - 2
    has_later = later < count
    has_earlier = earlier >= 0

    @pl.when(has_later)
    def _():
        pl.semaphore_signal(barrier, inc=1, device_id={"section": later}, device_id_type=MESH)

    rows = tokens_hbm.shape[0]
    head = gains_ref.shape[1]
    width = weight.shape[2]
    heads = width // head
    units = 2 * heads
    patch = 2 * rows

    factor = head ** (-0.5) * log2_e
    pair = 2 if heads % 2 == 0 else 1
    span = pair * head
    pairs = heads // pair
    lag = pair + 1
    back_lag = 3 * pair
    ready = 1
    groups = 2 * pairs

    def columns(step_index):
        return pl.ds(pl.multiple_of(step_index * span, span), span)

    def load(place, source, target):
        return pltpu.make_async_copy(source, target, load_sem.at[place])

    small = [
        load(place, source, target)
        for place, (source, target) in enumerate(
            (
                (modulation_hbm, modulation_ref),
                (gains_hbm, gains_ref),
            )
        )
    ]
    half_rows = rows // 2
    slabs = [slice(0, half_rows), slice(half_rows, rows)]
    token_loads = [
        load(2 + place, tokens_hbm.at[slab], tokens_ref.at[slab])
        for place, slab in enumerate(slabs)
    ]
    rest = width - span
    first_weights = load(4, weight_hbm.at[0, :, rest:width], weight.at[0, :, rest:width])
    other_weights = load(5, weight_hbm.at[0, :, 0:rest], weight.at[0, :, 0:rest])
    cache_weights = load(6, weight_hbm.at[1:3], weight.at[1:3])
    stale_load = load(7, stale_hbm, stale)
    text_load = load(8, text_hbm, text)
    keep_load = load(9, keep_hbm, keep_ref)
    order_load = load(10, order_hbm, order_ref)
    count_load = load(11, count_hbm, count_ref)
    last_row = max(rest - span, 0)
    output_loads = [
        load(12, output_weight_hbm.at[rest:width], output_weight.at[0:span]),
        load(13, output_weight_hbm.at[last_row : last_row + span], last_weight),
    ]
    if rest > 0:
        output_loads.append(
            load(14, output_weight_hbm.at[0:rest], output_weight.at[span:width])
        )
    token_loads[0].start()
    for copy in small:
        copy.start()
    first_weights.start()
    token_loads[1].start()
    if rest > 0:
        other_weights.start()

    def normalize(slab):
        hidden = tokens_ref[slab].astype(f32)
        shifted = hidden - jnp.mean(hidden, axis=-1, keepdims=True)
        spread = jnp.mean(shifted * shifted, axis=-1, keepdims=True)
        normed[0, slab] = (
            shifted * lax.rsqrt(spread + epsilon) * (1.0 + modulation_ref[1:2, :])
            + modulation_ref[0:1, :]
        ).astype(bf16)

    normed_copies = [
        pltpu.make_async_remote_copy(
            src_ref=normed.at[0, slab],
            dst_ref=normed.at[1, slab],
            send_sem=send_sem.at[0],
            recv_sem=normed_sem.at[place],
            device_id={"head": other_core},
            device_id_type=MESH,
        )
        for place, slab in enumerate(slabs)
    ]

    def remote(source, target, kind, sem, first, number, device):
        return pltpu.make_async_remote_copy(
            src_ref=source.at[pl.ds(first, number)],
            dst_ref=target.at[pl.ds(first, number)],
            send_sem=send_sem.at[kind],
            recv_sem=sem,
            device_id={"section": device},
            device_id_type=MESH,
        )

    def query_copy(group):
        return remote(query, query_mate, 1, query_sem.at[group + 1], group * pair, pair, mate)

    def first_copy(place):
        return pltpu.make_async_remote_copy(
            src_ref=query.at[0:pair, slabs[place]],
            dst_ref=query_mate.at[0:pair, slabs[place]],
            send_sem=send_sem.at[1],
            recv_sem=query_sem.at[place],
            device_id={"section": mate},
            device_id_type=MESH,
        )

    def forward_copy(unit, device):
        return remote(query_mate, query_far, 2, forward_sem.at[unit], unit, 1, device)

    def far_copy(unit, device):
        return remote(far_out, far_in, 3, far_sem.at[unit], unit, 1, device)

    def far_total_copy(group, device):
        return remote(
            far_total_out, far_total_in, 4, far_total_sem.at[group], group * pair, pair, device
        )

    def back_copy(group):
        return remote(back_out, back_in, 5, back_sem.at[group], group * pair, pair, mate)

    total_parts = [(0, pair + heads)]
    for first in range(pair + heads, units, pair):
        total_parts.append((first, pair))

    def back_total_copy(part):
        first, number = total_parts[part]
        return remote(
            back_total_out, back_total_in, 6, back_total_sem.at[part], first, number, mate
        )

    def sent(source, target, kind, axis, device):
        return pltpu.make_async_remote_copy(
            src_ref=source,
            dst_ref=target,
            send_sem=send_sem.at[kind],
            recv_sem=mixed_sem.at[0],
            device_id={axis: device},
            device_id_type=MESH,
        ).wait_send()

    def project_queries(half, c, first):
        part = jnp.dot(normed[half], weight[0, :, columns(c)], preferred_element_type=f32)
        for j in range(pair):
            query[first + j] = (
                head_norm(part[:, j * head : (j + 1) * head], gains_ref[0:1, :]) * factor
            ).astype(bf16)

    def forward(group):
        @pl.when(group == 0)
        def _():
            for place in range(2):
                first_copy(place).wait_recv()

        @pl.when(group > 0)
        def _():
            query_copy(group).wait_recv()

        @pl.when(has_ahead)
        def _():
            for j in range(pair):
                forward_copy(group * pair + j, ahead).start()

    def first_queries(place):
        slab = slabs[place]
        part = jnp.dot(
            normed[0, slab], weight[0, :, width - span : width], preferred_element_type=f32
        )
        for j in range(pair):
            query[j, slab] = (
                head_norm(part[:, j * head : (j + 1) * head], gains_ref[0:1, :]) * factor
            ).astype(bf16)

    def send_first(place):
        normed_copies[place].start()
        first_copy(place).start()

    token_loads[0].wait()
    for copy in small:
        copy.wait()
    normalize(slabs[0])
    first_weights.wait()
    first_queries(0)

    pl.semaphore_wait(barrier, 2 + has_earlier.astype(jnp.int32))

    @pl.when(has_earlier)
    def _():
        pl.semaphore_signal(
            present_sem, inc=1, device_id={"section": earlier}, device_id_type=MESH
        )

    send_first(0)
    token_loads[1].wait()
    normalize(slabs[1])
    first_queries(1)
    send_first(1)
    for copy in (cache_weights, stale_load, text_load, keep_load, order_load, count_load):
        copy.start()
    for copy in output_loads:
        copy.start()
    if rest > 0:
        other_weights.wait()

    @pl.loop(0, pairs - 1)
    def _(c):
        project_queries(0, c, pair + heads + c * pair)

    for copy in normed_copies:
        copy.wait_recv()

    @pl.loop(0, pairs)
    def _(c):
        project_queries(1, c, pair + c * pair)
        query_copy(1 + c).start()

    for c in range(pairs - 1):
        query_copy(1 + pairs + c).start()

    @pl.when(has_later)
    def _():
        pl.semaphore_wait(present_sem, 1)

    cache_weights.wait()
    own_rows = pl.ds(pl.multiple_of(core * rows, rows), rows)
    other_rows = pl.ds(pl.multiple_of(other_core * rows, rows), rows)

    @pl.loop(0, heads // pair)
    def _(c):
        for w in range(2):
            part = jnp.dot(
                normed[...].reshape(patch, normed.shape[2]),
                weight[1 + w, :, columns(c)],
                preferred_element_type=f32,
            ).astype(bf16)
            raw[w, own_rows, columns(c)] = part[0:rows]
            raw[w, other_rows, columns(c)] = part[rows:patch]

        @pl.when(c == min(1, pairs - 1))
        def _():
            forward(0)


    for copy in (stale_load, text_load, keep_load, order_load, count_load):
        copy.wait()

    keep_row = keep_ref[pl.ds(pl.multiple_of(me * patch, patch), patch)].astype(f32)
    keep = jnp.transpose(jnp.broadcast_to(keep_row[None, :], (head, patch)))
    text_rows = text.shape[1]
    live = (
        lax.broadcasted_iota(jnp.int32, (text_rows, head), 0) < count_ref[0]
    ).astype(f32)

    @pl.loop(0, heads)
    def _(h):
        lanes = pl.ds(pl.multiple_of(h * head, head), head)
        for version, cache in ((0, raw), (1, stale)):
            keys[version, h] = head_norm(
                cache[0, :, lanes].astype(f32), gains_ref[1:2, :]
            ).astype(bf16)
            values[version, h, :, 0:head] = (cache[1, :, lanes].astype(f32) * keep).astype(bf16)
            values[version, h, :, head : 2 * head] = keep.astype(bf16)
        text_keys[h] = head_norm(text[0, :, lanes].astype(f32), gains_ref[2:3, :]).astype(bf16)
        text_values[h, :, 0:head] = (text[1, :, lanes].astype(f32) * live).astype(bf16)
        text_values[h, :, head : 2 * head] = live.astype(bf16)

    own_slot = order_ref[me]
    mate_version = jnp.where(own_slot < order_ref[mate], 0, 1)
    far_patch = jnp.clip(me - 1 + 2 * parity, 0, count - 1)
    far_version = jnp.where(own_slot < order_ref[far_patch], 0, 1)

    def weighted(queries, key_rows, value_rows):
        weights = jnp.exp2(dot_nt(queries, key_rows)).astype(bf16)
        return jnp.dot(weights, value_rows, preferred_element_type=f32)

    def total_rows(summed):
        return jnp.transpose(summed[:, head : 2 * head])[0:1, :]

    def send_back(unit):
        numerator = mate_sum[unit, :, 0:head]
        last_of_pair = lax.rem(unit, pair) == pair - 1
        group = unit // pair

        @pl.when(has_ahead)
        def _():
            far_copy(unit, mate).wait_recv()
            back_out[unit] = (numerator + far_in[unit].astype(f32)).astype(bf16)

        @pl.when(jnp.logical_not(has_ahead))
        def _():
            back_out[unit] = numerator.astype(bf16)

        @pl.when(last_of_pair)
        def _():
            mine = [group * pair + j for j in range(pair)]

            @pl.when(has_ahead)
            def _():
                far_total_copy(group, mate).wait_recv()
                for one in mine:
                    back_total_out[one] = total_rows(mate_sum[one]) + far_total_in[one]

            @pl.when(jnp.logical_not(has_ahead))
            def _():
                for one in mine:
                    back_total_out[one] = total_rows(mate_sum[one])

            for part, (first, number) in enumerate(total_parts):

                @pl.when(unit == first + number - 1)
                def _():
                    back_total_copy(part).start()

            back_copy(group).start()

    @pl.loop(ready * pair, units + back_lag)
    def _(i):
        @pl.when(jnp.logical_and(i < units, lax.rem(i, pair) == 0))
        def _():
            forward(i // pair)

        unit = i - lag

        @pl.when(jnp.logical_and(unit >= 0, unit < units))
        def _():
            h = lax.rem(unit + heads - pair, heads)

            @pl.when(has_behind)
            def _():
                forward_copy(unit, mate).wait_recv()

            far = weighted(query_far[unit], keys[far_version, h], values[far_version, h])
            mate_sum[unit] = weighted(
                query_mate[unit], keys[mate_version, h], values[mate_version, h]
            )
            own_sum[unit] = weighted(query[unit], keys[0, h], values[0, h]) + weighted(
                query[unit], text_keys[h], text_values[h]
            )
            far_out[unit] = far[:, 0:head].astype(bf16)
            far_total_out[unit] = total_rows(far)

            @pl.when(has_behind)
            def _():
                far_copy(unit, behind).start()

                @pl.when(lax.rem(unit, pair) == pair - 1)
                def _():
                    far_total_copy(unit // pair, behind).start()

        @pl.when(i >= back_lag)
        def _():
            send_back(i - back_lag)

    def arrive(unit):
        back_copy(unit // pair).wait_recv()

    def gathered(unit):
        total = jnp.transpose(jnp.broadcast_to(back_total_in[unit], (head, rows)))
        mine = own_sum[unit]
        return (
            (mine[:, 0:head] + back_in[unit].astype(f32)) / (mine[:, head : 2 * head] + total)
        ).astype(bf16)

    def gather_range(half, first, last_unit, place):
        @pl.loop(0, (last_unit - first) // pair)
        def _(c):
            arrive(first + c * pair)
            for j in range(pair):
                lanes = pl.ds(pl.multiple_of((place + c * pair + j) * head, head), head)
                attended[half, :, lanes] = gathered(first + c * pair + j)

    mixed_copy = pltpu.make_async_remote_copy(
        src_ref=mixed_out,
        dst_ref=mixed_in,
        send_sem=send_sem.at[7],
        recv_sem=mixed_sem.at[0],
        device_id={"head": other_core},
        device_id_type=MESH,
    )
    full = output_weight.shape[1]
    wide = 512 if full % 512 == 0 else full

    for copy in output_loads:
        copy.wait()
    back_total_copy(0).wait_recv()
    gather_range(1, pair, pair + heads - pair, pair)
    gather_range(1, heads, pair + heads, 0)

    @pl.loop(0, full // wide)
    def _(c):
        here = pl.ds(pl.multiple_of(c * wide, wide), wide)
        mixed_out[:, here] = jnp.dot(
            attended[1], output_weight[:, here], preferred_element_type=f32
        ).astype(bf16)

    mixed_copy.start()
    gather_range(0, 0, pair, 0)
    for part in range(1, len(total_parts) - 1):
        first, number = total_parts[part]
        back_total_copy(part).wait_recv()
        gather_range(0, first, first + number, first - heads)
    most = width - span
    mixed_copy.wait_recv()

    @pl.loop(0, full // wide)
    def _(c):
        here = pl.ds(pl.multiple_of(c * wide, wide), wide)
        mixed = mixed_in[:, here].astype(f32) + jnp.dot(
            attended[0, :, 0:most], output_weight[0:most, here], preferred_element_type=f32
        )
        base[:, here] = tokens_ref[:, here].astype(f32) + modulation_ref[2:3, here] * mixed

    if len(total_parts) > 1:
        back_total_copy(len(total_parts) - 1).wait_recv()
    arrive(units - pair)
    for j in range(pair):
        last[:, j * head : (j + 1) * head] = gathered(units - pair + j)
    sent(normed.at[0], normed.at[1], 0, "head", other_core)
    mixed_copy.wait_send()
    sent(query, query_mate, 1, "section", mate)
    sent(back_out, back_in, 5, "section", mate)
    sent(back_total_out, back_total_in, 6, "section", mate)

    @pl.when(has_ahead)
    def _():
        sent(query_mate, query_far, 2, "section", mate)

    @pl.when(has_behind)
    def _():
        sent(far_out, far_in, 3, "section", mate)
        sent(far_total_out, far_total_in, 4, "section", mate)


def finish(base, last, last_weight, modulation, raw, updated_hbm, raw_hbm, updated, sems):
    full = base.shape[1]
    wide = 512 if full % 512 == 0 else full
    raw_copy = pltpu.make_async_copy(raw, raw_hbm, sems.at[0])
    raw_copy.start()
    copies = []
    for c in range(full // wide):
        here = slice(c * wide, (c + 1) * wide)
        updated[:, here] = (
            base[:, here]
            + modulation[2:3, here]
            * jnp.dot(last[...], last_weight[:, here], preferred_element_type=f32)
        ).astype(bf16)
        copies.append(
            pltpu.make_async_copy(updated.at[:, here], updated_hbm.at[:, here], sems.at[1 + c])
        )
        copies[c].start()
    for copy in copies:
        copy.wait()
    raw_copy.wait()


def on_device(
    video_tokens,
    modulation,
    project_weight,
    output_weight,
    norm_gains,
    text_cache,
    text_count,
    video_keep,
    patch_order,
    stale_cache,
):
    head = norm_gains.shape[1]
    rows, model = video_tokens.shape
    width = project_weight.shape[2]
    patch = stale_cache.shape[1]
    text_rows = text_cache.shape[1]
    heads = width // head
    units = 2 * heads
    pair = 2 if heads % 2 == 0 else 1
    pairs = heads // pair
    vmem = pl.BlockSpec(memory_space=pltpu.VMEM)
    hbm = pl.BlockSpec(memory_space=pl.ANY)
    unit_rows = pltpu.VMEM((units, rows, head), bf16)
    unit_totals = pltpu.VMEM((units, 1, rows), f32)
    unit_sums = pltpu.VMEM((units, rows, 2 * head), f32)
    handed = pl.pallas_call(
        kernel,
        out_shape=(
            pltpu.VMEM(video_tokens.shape, f32),
            pltpu.VMEM((rows, pair * head), bf16),
            pltpu.VMEM((pair * head, model), bf16),
            pltpu.VMEM(modulation.shape, f32),
            pltpu.VMEM(stale_cache.shape, bf16),
        ),
        in_specs=[hbm] * 10,
        out_specs=(vmem,) * 5,
        scratch_shapes=[
            pltpu.SMEM(patch_order.shape, jnp.int32),
            pltpu.SMEM(text_count.shape, jnp.int32),
            pltpu.VMEM(video_tokens.shape, bf16),
            pltpu.VMEM(norm_gains.shape, f32),
            pltpu.VMEM(video_keep.shape, jnp.int32),
            pltpu.VMEM(project_weight.shape, bf16),
            pltpu.VMEM(output_weight.shape, bf16),
            pltpu.VMEM(text_cache.shape, bf16),
            pltpu.VMEM(stale_cache.shape, bf16),
            pltpu.VMEM((2, rows, model), bf16),
            unit_rows,
            unit_rows,
            unit_rows,
            pltpu.VMEM((2, heads, patch, head), bf16),
            pltpu.VMEM((2, heads, patch, 2 * head), bf16),
            pltpu.VMEM((heads, text_rows, head), bf16),
            pltpu.VMEM((heads, text_rows, 2 * head), bf16),
            unit_sums,
            unit_sums,
            unit_rows,
            unit_totals,
            unit_rows,
            unit_totals,
            unit_rows,
            unit_totals,
            unit_rows,
            unit_totals,
            pltpu.VMEM((2, rows, width), bf16),
            pltpu.VMEM((rows, model), bf16),
            pltpu.VMEM((rows, model), bf16),
            pltpu.SemaphoreType.DMA((15,)),
            pltpu.SemaphoreType.DMA((8,)),
            pltpu.SemaphoreType.DMA((2,)),
            pltpu.SemaphoreType.DMA((2 * pairs + 1,)),
            pltpu.SemaphoreType.DMA((units,)),
            pltpu.SemaphoreType.DMA((units,)),
            pltpu.SemaphoreType.DMA((2 * pairs,)),
            pltpu.SemaphoreType.DMA((2 * pairs,)),
            pltpu.SemaphoreType.DMA((pairs,)),
            pltpu.SemaphoreType.DMA((1,)),
            pltpu.SemaphoreType.REGULAR,
        ],
        compiler_params=pltpu.CompilerParams(
            collective_id=0, has_side_effects=True, vmem_limit_bytes=52 * 1024 * 1024
        ),
    )(
        patch_order,
        text_count,
        video_tokens,
        modulation,
        norm_gains,
        video_keep,
        project_weight,
        output_weight,
        text_cache,
        stale_cache,
    )
    return pl.pallas_call(
        finish,
        out_shape=(
            jax.ShapeDtypeStruct(video_tokens.shape, bf16),
            jax.ShapeDtypeStruct(stale_cache.shape, bf16),
        ),
        in_specs=[vmem] * 5,
        out_specs=(hbm, hbm),
        scratch_shapes=[
            pltpu.VMEM(video_tokens.shape, bf16),
            pltpu.SemaphoreType.DMA((1 + model // (512 if model % 512 == 0 else model),)),
        ],
        compiler_params=pltpu.CompilerParams(vmem_limit_bytes=16 * 1024 * 1024),
    )(*[pltpu.with_memory_space_constraint(array, pltpu.VMEM) for array in handed])


def solution(mesh):
    placed = (
        P(("groups", "section", "head"), None),
        P("groups", None),
        P(None, None, "head"),
        P("head", None),
        P(),
        P(None, "groups", "head"),
        P("groups"),
        P("groups"),
        P("groups"),
        P(None, ("groups", "section"), "head"),
    )
    return jax.shard_map(
        on_device,
        mesh=mesh,
        in_specs=placed,
        out_specs=(P(("groups", "section", "head"), None), P(None, ("groups", "section"), "head")),
        check_vma=False,
    )
```

```python
import jax
import jax.numpy as jnp
from jax import lax
from jax.experimental import pallas as pl
from jax.experimental.pallas import tpu as pltpu
from jax.sharding import PartitionSpec as P

epsilon = 1e-06
log2_e = 1.4426950408889634
MESH = pl.DeviceIdType.MESH
f32 = jnp.float32
bf16 = jnp.bfloat16


def dot_nt(a, b):
    return lax.dot_general(a, b, (((1,), (1,)), ((), ())), preferred_element_type=f32)


def head_norm(rows, gain):
    return rows * lax.rsqrt(jnp.mean(rows * rows, axis=-1, keepdims=True) + epsilon) * gain


def kernel(
    order_hbm,
    count_hbm,
    tokens_hbm,
    modulation_hbm,
    gains_hbm,
    keep_hbm,
    weight_hbm,
    output_weight_hbm,
    text_hbm,
    stale_hbm,
    base,
    last,
    last_weight,
    modulation_ref,
    raw,
    order_ref,
    count_ref,
    tokens_ref,
    gains_ref,
    keep_ref,
    weight,
    output_weight,
    text,
    stale,
    normed,
    query,
    query_mate,
    query_far,
    keys,
    values,
    text_keys,
    text_values,
    own_sum,
    mate_sum,
    far_out,
    far_total_out,
    far_in,
    far_total_in,
    back_out,
    back_total_out,
    back_in,
    back_total_in,
    attended,
    mixed_out,
    mixed_in,
    load_sem,
    send_sem,
    normed_sem,
    query_sem,
    forward_sem,
    far_sem,
    far_total_sem,
    back_sem,
    back_total_sem,
    mixed_sem,
    present_sem,
):
    count = lax.axis_size("section")
    me = lax.axis_index("section")
    core = lax.axis_index("head")
    other_core = 1 - core
    parity = lax.rem(me, 2)
    mate = me + 1 - 2 * parity
    step = 2 - 4 * parity
    ahead = me + step
    behind = me - step
    has_ahead = jnp.logical_and(ahead >= 0, ahead < count)
    has_behind = jnp.logical_and(behind >= 0, behind < count)
    rows = tokens_hbm.shape[0]
    head = gains_ref.shape[1]
    width = weight.shape[2]
    heads = width // head
    units = 2 * heads
    patch = 2 * rows

    factor = head ** (-0.5) * log2_e
    pair = 2 if heads % 2 == 0 else 1
    span = pair * head
    pairs = heads // pair
    lag = pair + 1
    back_lag = 3 * pair
    own_lag = 3 * pair
    ready = 1
    groups = 2 * pairs

    def columns(step_index):
        return pl.ds(pl.multiple_of(step_index * span, span), span)

    def load(place, source, target):
        return pltpu.make_async_copy(source, target, load_sem.at[place])

    small = [
        load(place, source, target)
        for place, (source, target) in enumerate(
            (
                (modulation_hbm, modulation_ref),
                (gains_hbm, gains_ref),
            )
        )
    ]
    half_rows = rows // 2
    slabs = [slice(0, half_rows), slice(half_rows, rows)]
    token_loads = [
        load(2 + place, tokens_hbm.at[slab], tokens_ref.at[slab])
        for place, slab in enumerate(slabs)
    ]
    rest = width - span
    first_weights = load(4, weight_hbm.at[0, :, rest:width], weight.at[0, :, rest:width])
    other_weights = load(5, weight_hbm.at[0, :, 0:rest], weight.at[0, :, 0:rest])
    cache_weights = load(6, weight_hbm.at[1:3], weight.at[1:3])
    stale_load = load(7, stale_hbm, stale)
    text_load = load(8, text_hbm, text)
    keep_load = load(9, keep_hbm, keep_ref)
    order_load = load(10, order_hbm, order_ref)
    count_load = load(11, count_hbm, count_ref)
    last_row = max(rest - span, 0)
    output_loads = [
        load(12, output_weight_hbm.at[rest:width], output_weight.at[0:span]),
        load(13, output_weight_hbm.at[last_row : last_row + span], last_weight),
    ]
    if rest > 0:
        output_loads.append(
            load(14, output_weight_hbm.at[0:rest], output_weight.at[span:width])
        )
    token_loads[0].start()

    barrier = pltpu.get_barrier_semaphore()
    pl.semaphore_signal(barrier, inc=1, device_id={"head": other_core}, device_id_type=MESH)
    pl.semaphore_signal(barrier, inc=1, device_id={"section": mate}, device_id_type=MESH)

    later = me + 2
    earlier = me - 2
    has_later = later < count
    has_earlier = earlier >= 0

    @pl.when(has_later)
    def _():
        pl.semaphore_signal(barrier, inc=1, device_id={"section": later}, device_id_type=MESH)

    for copy in small:
        copy.start()
    first_weights.start()
    token_loads[1].start()
    if rest > 0:
        other_weights.start()

    def normalize(slab):
        hidden = tokens_ref[slab].astype(f32)
        shifted = hidden - jnp.mean(hidden, axis=-1, keepdims=True)
        spread = jnp.mean(shifted * shifted, axis=-1, keepdims=True)
        normed[0, slab] = (
            shifted * lax.rsqrt(spread + epsilon) * (1.0 + modulation_ref[1:2, :])
            + modulation_ref[0:1, :]
        ).astype(bf16)

    normed_copies = [
        pltpu.make_async_remote_copy(
            src_ref=normed.at[0, slab],
            dst_ref=normed.at[1, slab],
            send_sem=send_sem.at[0],
            recv_sem=normed_sem.at[place],
            device_id={"head": other_core},
            device_id_type=MESH,
        )
        for place, slab in enumerate(slabs)
    ]

    def remote(source, target, kind, sem, first, number, device):
        return pltpu.make_async_remote_copy(
            src_ref=source.at[pl.ds(first, number)],
            dst_ref=target.at[pl.ds(first, number)],
            send_sem=send_sem.at[kind],
            recv_sem=sem,
            device_id={"section": device},
            device_id_type=MESH,
        )

    def query_copy(group):
        return remote(query, query_mate, 1, query_sem.at[group + 1], group * pair, pair, mate)

    def first_copy(place):
        return pltpu.make_async_remote_copy(
            src_ref=query.at[0:pair, slabs[place]],
            dst_ref=query_mate.at[0:pair, slabs[place]],
            send_sem=send_sem.at[1],
            recv_sem=query_sem.at[place],
            device_id={"section": mate},
            device_id_type=MESH,
        )

    def forward_copy(unit, device):
        return remote(query_mate, query_far, 2, forward_sem.at[unit], unit, 1, device)

    def far_copy(unit, device):
        return remote(far_out, far_in, 3, far_sem.at[unit], unit, 1, device)

    def far_total_copy(group, device):
        return remote(
            far_total_out, far_total_in, 4, far_total_sem.at[group], group * pair, pair, device
        )

    def back_copy(group):
        return remote(back_out, back_in, 5, back_sem.at[group], group * pair, pair, mate)

    total_parts = [(0, pair + heads)]
    for first in range(pair + heads, units, pair):
        total_parts.append((first, pair))

    def back_total_copy(part):
        first, number = total_parts[part]
        return remote(
            back_total_out, back_total_in, 6, back_total_sem.at[part], first, number, mate
        )

    def sent(source, target, kind, axis, device):
        return pltpu.make_async_remote_copy(
            src_ref=source,
            dst_ref=target,
            send_sem=send_sem.at[kind],
            recv_sem=mixed_sem.at[0],
            device_id={axis: device},
            device_id_type=MESH,
        ).wait_send()

    def project_queries(half, c, first):
        part = jnp.dot(normed[half], weight[0, :, columns(c)], preferred_element_type=f32)
        for j in range(pair):
            query[first + j] = (
                head_norm(part[:, j * head : (j + 1) * head], gains_ref[0:1, :]) * factor
            ).astype(bf16)

    def forward(group):
        @pl.when(group == 0)
        def _():
            for place in range(2):
                first_copy(place).wait_recv()

        @pl.when(group > 0)
        def _():
            query_copy(group).wait_recv()

        @pl.when(has_ahead)
        def _():
            for j in range(pair):
                forward_copy(group * pair + j, ahead).start()

    def first_queries(place):
        slab = slabs[place]
        part = jnp.dot(
            normed[0, slab], weight[0, :, width - span : width], preferred_element_type=f32
        )
        for j in range(pair):
            query[j, slab] = (
                head_norm(part[:, j * head : (j + 1) * head], gains_ref[0:1, :]) * factor
            ).astype(bf16)

    token_loads[0].wait()
    for copy in small:
        copy.wait()
    normalize(slabs[0])
    first_weights.wait()
    first_queries(0)

    pl.semaphore_wait(barrier, 2 + has_earlier.astype(jnp.int32))

    @pl.when(has_earlier)
    def _():
        pl.semaphore_signal(
            present_sem, inc=1, device_id={"section": earlier}, device_id_type=MESH
        )

    normed_copies[0].start()
    first_copy(0).start()
    token_loads[1].wait()
    normalize(slabs[1])
    normed_copies[1].start()
    first_queries(1)
    first_copy(1).start()
    for copy in (cache_weights, stale_load, text_load, keep_load, order_load, count_load):
        copy.start()
    for copy in output_loads:
        copy.start()
    if rest > 0:
        other_weights.wait()

    @pl.loop(0, pairs - 1)
    def _(c):
        project_queries(0, c, pair + heads + c * pair)

    for copy in normed_copies:
        copy.wait_recv()

    @pl.loop(0, pairs)
    def _(c):
        project_queries(1, c, pair + c * pair)
        query_copy(1 + c).start()

    for c in range(pairs - 1):
        query_copy(1 + pairs + c).start()

    @pl.when(has_later)
    def _():
        pl.semaphore_wait(present_sem, 1)

    cache_weights.wait()
    own_rows = pl.ds(pl.multiple_of(core * rows, rows), rows)
    other_rows = pl.ds(pl.multiple_of(other_core * rows, rows), rows)

    @pl.loop(0, heads // pair)
    def _(c):
        for w in range(2):
            part = jnp.dot(
                normed[...].reshape(patch, normed.shape[2]),
                weight[1 + w, :, columns(c)],
                preferred_element_type=f32,
            ).astype(bf16)
            raw[w, own_rows, columns(c)] = part[0:rows]
            raw[w, other_rows, columns(c)] = part[rows:patch]

        @pl.when(c == min(1, pairs - 1))
        def _():
            forward(0)


    for copy in (stale_load, text_load, keep_load, order_load, count_load):
        copy.wait()

    keep_row = keep_ref[pl.ds(pl.multiple_of(me * patch, patch), patch)].astype(f32)
    keep = jnp.transpose(jnp.broadcast_to(keep_row[None, :], (head, patch)))
    text_rows = text.shape[1]
    live = (
        lax.broadcasted_iota(jnp.int32, (text_rows, head), 0) < count_ref[0]
    ).astype(f32)

    @pl.loop(0, heads)
    def _(h):
        lanes = pl.ds(pl.multiple_of(h * head, head), head)
        for version, cache in ((0, raw), (1, stale)):
            keys[version, h] = head_norm(
                cache[0, :, lanes].astype(f32), gains_ref[1:2, :]
            ).astype(bf16)
            values[version, h, :, 0:head] = (cache[1, :, lanes].astype(f32) * keep).astype(bf16)
            values[version, h, :, head : 2 * head] = keep.astype(bf16)
        text_keys[h] = head_norm(text[0, :, lanes].astype(f32), gains_ref[2:3, :]).astype(bf16)
        text_values[h, :, 0:head] = (text[1, :, lanes].astype(f32) * live).astype(bf16)
        text_values[h, :, head : 2 * head] = live.astype(bf16)

    own_slot = order_ref[me]
    mate_version = jnp.where(own_slot < order_ref[mate], 0, 1)
    far_patch = jnp.clip(me - 1 + 2 * parity, 0, count - 1)
    far_version = jnp.where(own_slot < order_ref[far_patch], 0, 1)

    def weighted(queries, key_rows, value_rows):
        weights = jnp.exp2(dot_nt(queries, key_rows)).astype(bf16)
        return jnp.dot(weights, value_rows, preferred_element_type=f32)

    def head_of(unit):
        return lax.rem(unit + heads - pair, heads)

    def total_rows(summed):
        return jnp.transpose(summed[:, head : 2 * head])[0:1, :]

    def send_back(unit):
        numerator = mate_sum[unit, :, 0:head]
        last_of_pair = lax.rem(unit, pair) == pair - 1
        group = unit // pair

        @pl.when(has_ahead)
        def _():
            far_copy(unit, mate).wait_recv()
            back_out[unit] = (numerator + far_in[unit].astype(f32)).astype(bf16)

        @pl.when(jnp.logical_not(has_ahead))
        def _():
            back_out[unit] = numerator.astype(bf16)

        @pl.when(last_of_pair)
        def _():
            mine = [group * pair + j for j in range(pair)]

            @pl.when(has_ahead)
            def _():
                far_total_copy(group, mate).wait_recv()
                for one in mine:
                    back_total_out[one] = total_rows(mate_sum[one]) + far_total_in[one]

            @pl.when(jnp.logical_not(has_ahead))
            def _():
                for one in mine:
                    back_total_out[one] = total_rows(mate_sum[one])

            for part, (first, number) in enumerate(total_parts):

                @pl.when(unit == first + number - 1)
                def _():
                    back_total_copy(part).start()

            back_copy(group).start()

    @pl.loop(ready * pair, units + max(back_lag, own_lag))
    def _(i):
        @pl.when(jnp.logical_and(i < units, lax.rem(i, pair) == 0))
        def _():
            forward(i // pair)

        unit = i - lag

        @pl.when(jnp.logical_and(unit >= 0, unit < units))
        def _():
            h = head_of(unit)

            @pl.when(has_behind)
            def _():
                forward_copy(unit, mate).wait_recv()

            far = weighted(query_far[unit], keys[far_version, h], values[far_version, h])
            mate_sum[unit] = weighted(
                query_mate[unit], keys[mate_version, h], values[mate_version, h]
            )
            far_out[unit] = far[:, 0:head].astype(bf16)
            far_total_out[unit] = total_rows(far)

            @pl.when(has_behind)
            def _():
                far_copy(unit, behind).start()

                @pl.when(lax.rem(unit, pair) == pair - 1)
                def _():
                    far_total_copy(unit // pair, behind).start()

        @pl.when(jnp.logical_and(i >= back_lag, i < units + back_lag))
        def _():
            send_back(i - back_lag)

        own = i - own_lag

        @pl.when(own >= 0)
        def _():
            h = head_of(own)
            own_sum[own] = weighted(query[own], keys[0, h], values[0, h]) + weighted(
                query[own], text_keys[h], text_values[h]
            )

    def arrive(unit):
        back_copy(unit // pair).wait_recv()

    def gathered(unit):
        total = jnp.transpose(jnp.broadcast_to(back_total_in[unit], (head, rows)))
        mine = own_sum[unit]
        return (
            (mine[:, 0:head] + back_in[unit].astype(f32)) / (mine[:, head : 2 * head] + total)
        ).astype(bf16)

    def gather_range(half, first, last_unit, place):
        @pl.loop(0, (last_unit - first) // pair)
        def _(c):
            arrive(first + c * pair)
            for j in range(pair):
                lanes = pl.ds(pl.multiple_of((place + c * pair + j) * head, head), head)
                attended[half, :, lanes] = gathered(first + c * pair + j)

    mixed_copy = pltpu.make_async_remote_copy(
        src_ref=mixed_out,
        dst_ref=mixed_in,
        send_sem=send_sem.at[7],
        recv_sem=mixed_sem.at[0],
        device_id={"head": other_core},
        device_id_type=MESH,
    )
    full = output_weight.shape[1]
    wide = 512 if full % 512 == 0 else full

    for copy in output_loads:
        copy.wait()
    back_total_copy(0).wait_recv()
    gather_range(1, pair, pair + heads - pair, pair)
    gather_range(1, heads, pair + heads, 0)

    @pl.loop(0, full // wide)
    def _(c):
        here = pl.ds(pl.multiple_of(c * wide, wide), wide)
        mixed_out[:, here] = jnp.dot(
            attended[1], output_weight[:, here], preferred_element_type=f32
        ).astype(bf16)

    mixed_copy.start()
    gather_range(0, 0, pair, 0)
    for part in range(1, len(total_parts) - 1):
        first, number = total_parts[part]
        back_total_copy(part).wait_recv()
        gather_range(0, first, first + number, first - heads)
    most = width - span
    mixed_copy.wait_recv()

    @pl.loop(0, full // wide)
    def _(c):
        here = pl.ds(pl.multiple_of(c * wide, wide), wide)
        mixed = mixed_in[:, here].astype(f32) + jnp.dot(
            attended[0, :, 0:most], output_weight[0:most, here], preferred_element_type=f32
        )
        base[:, here] = tokens_ref[:, here].astype(f32) + modulation_ref[2:3, here] * mixed

    if len(total_parts) > 1:
        back_total_copy(len(total_parts) - 1).wait_recv()
    arrive(units - pair)
    for j in range(pair):
        last[:, j * head : (j + 1) * head] = gathered(units - pair + j)
    sent(normed.at[0], normed.at[1], 0, "head", other_core)
    mixed_copy.wait_send()
    sent(query, query_mate, 1, "section", mate)
    sent(back_out, back_in, 5, "section", mate)
    sent(back_total_out, back_total_in, 6, "section", mate)

    @pl.when(has_ahead)
    def _():
        sent(query_mate, query_far, 2, "section", mate)

    @pl.when(has_behind)
    def _():
        sent(far_out, far_in, 3, "section", mate)
        sent(far_total_out, far_total_in, 4, "section", mate)


def finish(base, last, last_weight, modulation, raw, updated_hbm, raw_hbm, updated, sems):
    full = base.shape[1]
    wide = 512 if full % 512 == 0 else full
    raw_copy = pltpu.make_async_copy(raw, raw_hbm, sems.at[0])
    raw_copy.start()
    copies = []
    for c in range(full // wide):
        here = slice(c * wide, (c + 1) * wide)
        updated[:, here] = (
            base[:, here]
            + modulation[2:3, here]
            * jnp.dot(last[...], last_weight[:, here], preferred_element_type=f32)
        ).astype(bf16)
        copies.append(
            pltpu.make_async_copy(updated.at[:, here], updated_hbm.at[:, here], sems.at[1 + c])
        )
        copies[c].start()
    for copy in copies:
        copy.wait()
    raw_copy.wait()


def on_device(
    video_tokens,
    modulation,
    project_weight,
    output_weight,
    norm_gains,
    text_cache,
    text_count,
    video_keep,
    patch_order,
    stale_cache,
):
    head = norm_gains.shape[1]
    rows, model = video_tokens.shape
    width = project_weight.shape[2]
    patch = stale_cache.shape[1]
    text_rows = text_cache.shape[1]
    heads = width // head
    units = 2 * heads
    pair = 2 if heads % 2 == 0 else 1
    pairs = heads // pair
    vmem = pl.BlockSpec(memory_space=pltpu.VMEM)
    hbm = pl.BlockSpec(memory_space=pl.ANY)
    unit_rows = pltpu.VMEM((units, rows, head), bf16)
    unit_totals = pltpu.VMEM((units, 1, rows), f32)
    unit_sums = pltpu.VMEM((units, rows, 2 * head), f32)
    handed = pl.pallas_call(
        kernel,
        out_shape=(
            pltpu.VMEM(video_tokens.shape, f32),
            pltpu.VMEM((rows, pair * head), bf16),
            pltpu.VMEM((pair * head, model), bf16),
            pltpu.VMEM(modulation.shape, f32),
            pltpu.VMEM(stale_cache.shape, bf16),
        ),
        in_specs=[hbm] * 10,
        out_specs=(vmem,) * 5,
        scratch_shapes=[
            pltpu.SMEM(patch_order.shape, jnp.int32),
            pltpu.SMEM(text_count.shape, jnp.int32),
            pltpu.VMEM(video_tokens.shape, bf16),
            pltpu.VMEM(norm_gains.shape, f32),
            pltpu.VMEM(video_keep.shape, jnp.int32),
            pltpu.VMEM(project_weight.shape, bf16),
            pltpu.VMEM(output_weight.shape, bf16),
            pltpu.VMEM(text_cache.shape, bf16),
            pltpu.VMEM(stale_cache.shape, bf16),
            pltpu.VMEM((2, rows, model), bf16),
            unit_rows,
            unit_rows,
            unit_rows,
            pltpu.VMEM((2, heads, patch, head), bf16),
            pltpu.VMEM((2, heads, patch, 2 * head), bf16),
            pltpu.VMEM((heads, text_rows, head), bf16),
            pltpu.VMEM((heads, text_rows, 2 * head), bf16),
            unit_sums,
            unit_sums,
            unit_rows,
            unit_totals,
            unit_rows,
            unit_totals,
            unit_rows,
            unit_totals,
            unit_rows,
            unit_totals,
            pltpu.VMEM((2, rows, width), bf16),
            pltpu.VMEM((rows, model), bf16),
            pltpu.VMEM((rows, model), bf16),
            pltpu.SemaphoreType.DMA((15,)),
            pltpu.SemaphoreType.DMA((8,)),
            pltpu.SemaphoreType.DMA((2,)),
            pltpu.SemaphoreType.DMA((2 * pairs + 1,)),
            pltpu.SemaphoreType.DMA((units,)),
            pltpu.SemaphoreType.DMA((units,)),
            pltpu.SemaphoreType.DMA((2 * pairs,)),
            pltpu.SemaphoreType.DMA((2 * pairs,)),
            pltpu.SemaphoreType.DMA((pairs,)),
            pltpu.SemaphoreType.DMA((1,)),
            pltpu.SemaphoreType.REGULAR,
        ],
        compiler_params=pltpu.CompilerParams(
            collective_id=0, has_side_effects=True, vmem_limit_bytes=52 * 1024 * 1024
        ),
    )(
        patch_order,
        text_count,
        video_tokens,
        modulation,
        norm_gains,
        video_keep,
        project_weight,
        output_weight,
        text_cache,
        stale_cache,
    )
    return pl.pallas_call(
        finish,
        out_shape=(
            jax.ShapeDtypeStruct(video_tokens.shape, bf16),
            jax.ShapeDtypeStruct(stale_cache.shape, bf16),
        ),
        in_specs=[vmem] * 5,
        out_specs=(hbm, hbm),
        scratch_shapes=[
            pltpu.VMEM(video_tokens.shape, bf16),
            pltpu.SemaphoreType.DMA((1 + model // (512 if model % 512 == 0 else model),)),
        ],
        compiler_params=pltpu.CompilerParams(vmem_limit_bytes=16 * 1024 * 1024),
    )(*[pltpu.with_memory_space_constraint(array, pltpu.VMEM) for array in handed])


def solution(mesh):
    placed = (
        P(("groups", "section", "head"), None),
        P("groups", None),
        P(None, None, "head"),
        P("head", None),
        P(),
        P(None, "groups", "head"),
        P("groups"),
        P("groups"),
        P("groups"),
        P(None, ("groups", "section"), "head"),
    )
    return jax.shard_map(
        on_device,
        mesh=mesh,
        in_specs=placed,
        out_specs=(P(("groups", "section", "head"), None), P(None, ("groups", "section"), "head")),
        check_vma=False,
    )
```

```python
import jax
import jax.numpy as jnp
from jax import lax
from jax.experimental import pallas as pl
from jax.experimental.pallas import tpu as pltpu
from jax.sharding import PartitionSpec as P

epsilon = 1e-06
log2_e = 1.4426950408889634
MESH = pl.DeviceIdType.MESH
f32 = jnp.float32
bf16 = jnp.bfloat16


def dot_nt(a, b):
    return lax.dot_general(a, b, (((1,), (1,)), ((), ())), preferred_element_type=f32)


def head_norm(rows, gain):
    return rows * lax.rsqrt(jnp.mean(rows * rows, axis=-1, keepdims=True) + epsilon) * gain


def kernel(
    order_hbm,
    count_ref,
    tokens_hbm,
    modulation_hbm,
    gains_hbm,
    keep_hbm,
    weight_hbm,
    output_weight_hbm,
    text_hbm,
    stale_hbm,
    base,
    last,
    last_weight,
    modulation_ref,
    raw,
    order_ref,
    tokens_ref,
    gains_ref,
    keep_ref,
    weight,
    output_weight,
    text,
    stale,
    normed,
    query,
    query_mate,
    query_far,
    keys,
    values,
    text_keys,
    text_values,
    own_sum,
    mate_sum,
    far_out,
    far_total_out,
    far_in,
    far_total_in,
    back_out,
    back_total_out,
    back_in,
    back_total_in,
    attended,
    mixed_out,
    mixed_in,
    load_sem,
    send_sem,
    normed_sem,
    query_sem,
    forward_sem,
    far_sem,
    far_total_sem,
    back_sem,
    back_total_sem,
    mixed_sem,
    present_sem,
):
    count = lax.axis_size("section")
    me = lax.axis_index("section")
    core = lax.axis_index("head")
    other_core = 1 - core
    parity = lax.rem(me, 2)
    mate = me + 1 - 2 * parity
    step = 2 - 4 * parity
    ahead = me + step
    behind = me - step
    has_ahead = jnp.logical_and(ahead >= 0, ahead < count)
    has_behind = jnp.logical_and(behind >= 0, behind < count)
    rows = tokens_hbm.shape[0]
    head = gains_ref.shape[1]
    width = weight.shape[2]
    heads = width // head
    units = 2 * heads
    patch = 2 * rows

    factor = head ** (-0.5) * log2_e
    pair = 2 if heads % 2 == 0 else 1
    span = pair * head
    pairs = heads // pair
    lag = pair + 1
    back_lag = 3 * pair
    own_lag = 3 * pair
    ready = 1

    def columns(step_index):
        return pl.ds(pl.multiple_of(step_index * span, span), span)

    def load(place, source, target):
        return pltpu.make_async_copy(source, target, load_sem.at[place])

    small = [
        load(place, source, target)
        for place, (source, target) in enumerate(
            (
                (modulation_hbm, modulation_ref),
                (gains_hbm, gains_ref),
            )
        )
    ]
    half_rows = rows // 2
    slabs = [slice(0, half_rows), slice(half_rows, rows)]
    token_loads = [
        load(2 + place, tokens_hbm.at[slab], tokens_ref.at[slab])
        for place, slab in enumerate(slabs)
    ]
    rest = width - span
    first_weights = load(4, weight_hbm.at[0, :, rest:width], weight.at[0, :, rest:width])
    other_weights = load(5, weight_hbm.at[0, :, 0:rest], weight.at[0, :, 0:rest])
    cache_weights = load(6, weight_hbm.at[1:3], weight.at[1:3])
    stale_load = load(7, stale_hbm, stale)
    text_load = load(8, text_hbm, text)
    keep_load = load(9, keep_hbm, keep_ref)
    order_load = load(10, order_hbm, order_ref)
    last_row = max(rest - span, 0)
    output_loads = [
        load(11, output_weight_hbm.at[rest:width], output_weight.at[0:span]),
        load(12, output_weight_hbm.at[last_row : last_row + span], last_weight),
    ]
    if rest > 0:
        output_loads.append(
            load(13, output_weight_hbm.at[0:rest], output_weight.at[span:width])
        )
    token_loads[0].start()

    barrier = pltpu.get_barrier_semaphore()
    pl.semaphore_signal(barrier, inc=1, device_id={"head": other_core}, device_id_type=MESH)
    pl.semaphore_signal(barrier, inc=1, device_id={"section": mate}, device_id_type=MESH)

    later = me + 2
    earlier = me - 2
    has_later = later < count
    has_earlier = earlier >= 0

    @pl.when(has_later)
    def _():
        pl.semaphore_signal(barrier, inc=1, device_id={"section": later}, device_id_type=MESH)

    for copy in small:
        copy.start()
    first_weights.start()
    token_loads[1].start()

    def normalize(slab):
        hidden = tokens_ref[slab].astype(f32)
        shifted = hidden - jnp.mean(hidden, axis=-1, keepdims=True)
        spread = jnp.mean(shifted * shifted, axis=-1, keepdims=True)
        normed[0, slab] = (
            shifted * lax.rsqrt(spread + epsilon) * (1.0 + modulation_ref[1:2, :])
            + modulation_ref[0:1, :]
        ).astype(bf16)

    normed_copies = [
        pltpu.make_async_remote_copy(
            src_ref=normed.at[0, slab],
            dst_ref=normed.at[1, slab],
            send_sem=send_sem.at[0],
            recv_sem=normed_sem.at[place],
            device_id={"head": other_core},
            device_id_type=MESH,
        )
        for place, slab in enumerate(slabs)
    ]

    def remote(source, target, kind, sem, first, number, device):
        return pltpu.make_async_remote_copy(
            src_ref=source.at[pl.ds(first, number)],
            dst_ref=target.at[pl.ds(first, number)],
            send_sem=send_sem.at[kind],
            recv_sem=sem,
            device_id={"section": device},
            device_id_type=MESH,
        )

    def query_copy(group):
        return remote(query, query_mate, 1, query_sem.at[group + 1], group * pair, pair, mate)

    def first_copy(place):
        return pltpu.make_async_remote_copy(
            src_ref=query.at[0:pair, slabs[place]],
            dst_ref=query_mate.at[0:pair, slabs[place]],
            send_sem=send_sem.at[1],
            recv_sem=query_sem.at[place],
            device_id={"section": mate},
            device_id_type=MESH,
        )

    def forward_copy(unit, device):
        return remote(query_mate, query_far, 2, forward_sem.at[unit], unit, 1, device)

    def far_copy(unit, device):
        return remote(far_out, far_in, 3, far_sem.at[unit], unit, 1, device)

    def far_total_copy(group, device):
        return remote(
            far_total_out, far_total_in, 4, far_total_sem.at[group], group * pair, pair, device
        )

    def back_copy(group):
        return remote(back_out, back_in, 5, back_sem.at[group], group * pair, pair, mate)

    total_parts = [(0, pair + heads)]
    for first in range(pair + heads, units, pair):
        total_parts.append((first, pair))

    def back_total_copy(part):
        first, number = total_parts[part]
        return remote(
            back_total_out, back_total_in, 6, back_total_sem.at[part], first, number, mate
        )

    def sent(source, target, kind, axis, device):
        return pltpu.make_async_remote_copy(
            src_ref=source,
            dst_ref=target,
            send_sem=send_sem.at[kind],
            recv_sem=mixed_sem.at[0],
            device_id={axis: device},
            device_id_type=MESH,
        ).wait_send()

    def project_queries(half, c, first):
        part = jnp.dot(normed[half], weight[0, :, columns(c)], preferred_element_type=f32)
        for j in range(pair):
            query[first + j] = (
                head_norm(part[:, j * head : (j + 1) * head], gains_ref[0:1, :]) * factor
            ).astype(bf16)

    def forward(group):
        @pl.when(group == 0)
        def _():
            for place in range(2):
                first_copy(place).wait_recv()

        @pl.when(group > 0)
        def _():
            query_copy(group).wait_recv()

        @pl.when(has_ahead)
        def _():
            for j in range(pair):
                forward_copy(group * pair + j, ahead).start()

    def first_queries(place):
        slab = slabs[place]
        part = jnp.dot(
            normed[0, slab], weight[0, :, width - span : width], preferred_element_type=f32
        )
        for j in range(pair):
            query[j, slab] = (
                head_norm(part[:, j * head : (j + 1) * head], gains_ref[0:1, :]) * factor
            ).astype(bf16)

    token_loads[0].wait()
    for copy in small:
        copy.wait()
    if rest > 0:
        other_weights.start()
    normalize(slabs[0])
    first_weights.wait()
    first_queries(0)

    pl.semaphore_wait(barrier, 2 + has_earlier.astype(jnp.int32))

    @pl.when(has_earlier)
    def _():
        pl.semaphore_signal(
            present_sem, inc=1, device_id={"section": earlier}, device_id_type=MESH
        )

    normed_copies[0].start()
    first_copy(0).start()
    token_loads[1].wait()
    normalize(slabs[1])
    normed_copies[1].start()
    first_queries(1)
    first_copy(1).start()
    for copy in (cache_weights, stale_load, text_load, keep_load, order_load):
        copy.start()
    for copy in output_loads:
        copy.start()
    if rest > 0:
        other_weights.wait()

    @pl.loop(0, pairs - 1)
    def _(c):
        project_queries(0, c, pair + heads + c * pair)

    for copy in normed_copies:
        copy.wait_recv()

    @pl.loop(0, pairs)
    def _(c):
        project_queries(1, c, pair + c * pair)
        query_copy(1 + c).start()

    for c in range(pairs - 1):
        query_copy(1 + pairs + c).start()

    @pl.when(has_later)
    def _():
        pl.semaphore_wait(present_sem, 1)

    cache_weights.wait()
    own_rows = pl.ds(pl.multiple_of(core * rows, rows), rows)
    other_rows = pl.ds(pl.multiple_of(other_core * rows, rows), rows)

    @pl.loop(0, heads // pair)
    def _(c):
        for w in range(2):
            part = jnp.dot(
                normed[...].reshape(patch, normed.shape[2]),
                weight[1 + w, :, columns(c)],
                preferred_element_type=f32,
            ).astype(bf16)
            raw[w, own_rows, columns(c)] = part[0:rows]
            raw[w, other_rows, columns(c)] = part[rows:patch]

        @pl.when(c == min(1, pairs - 1))
        def _():
            forward(0)


    for copy in (stale_load, text_load, keep_load, order_load):
        copy.wait()

    keep_row = keep_ref[pl.ds(pl.multiple_of(me * patch, patch), patch)].astype(f32)
    keep = jnp.transpose(jnp.broadcast_to(keep_row[None, :], (head, patch)))
    text_rows = text.shape[1]
    live = (
        lax.broadcasted_iota(jnp.int32, (text_rows, head), 0) < count_ref[0]
    ).astype(f32)

    @pl.loop(0, heads)
    def _(h):
        lanes = pl.ds(pl.multiple_of(h * head, head), head)
        for version, cache in ((0, raw), (1, stale)):
            keys[version, h] = head_norm(
                cache[0, :, lanes].astype(f32), gains_ref[1:2, :]
            ).astype(bf16)
            values[version, h, :, 0:head] = (cache[1, :, lanes].astype(f32) * keep).astype(bf16)
            values[version, h, :, head : 2 * head] = keep.astype(bf16)
        text_keys[h] = head_norm(text[0, :, lanes].astype(f32), gains_ref[2:3, :]).astype(bf16)
        text_values[h, :, 0:head] = (text[1, :, lanes].astype(f32) * live).astype(bf16)
        text_values[h, :, head : 2 * head] = live.astype(bf16)

    own_slot = order_ref[me]
    mate_version = jnp.where(own_slot < order_ref[mate], 0, 1)
    far_patch = jnp.clip(me - 1 + 2 * parity, 0, count - 1)
    far_version = jnp.where(own_slot < order_ref[far_patch], 0, 1)

    def weighted(queries, key_rows, value_rows):
        weights = jnp.exp2(dot_nt(queries, key_rows)).astype(bf16)
        return jnp.dot(weights, value_rows, preferred_element_type=f32)

    def head_of(unit):
        return lax.rem(unit + heads - pair, heads)

    def total_rows(summed):
        return jnp.transpose(summed[:, head : 2 * head])[0:1, :]

    def send_back(unit):
        numerator = mate_sum[unit, :, 0:head]
        last_of_pair = lax.rem(unit, pair) == pair - 1
        group = unit // pair

        @pl.when(has_ahead)
        def _():
            far_copy(unit, mate).wait_recv()
            back_out[unit] = (numerator + far_in[unit].astype(f32)).astype(bf16)

        @pl.when(jnp.logical_not(has_ahead))
        def _():
            back_out[unit] = numerator.astype(bf16)

        @pl.when(last_of_pair)
        def _():
            mine = [group * pair + j for j in range(pair)]

            @pl.when(has_ahead)
            def _():
                far_total_copy(group, mate).wait_recv()
                for one in mine:
                    back_total_out[one] = total_rows(mate_sum[one]) + far_total_in[one]

            @pl.when(jnp.logical_not(has_ahead))
            def _():
                for one in mine:
                    back_total_out[one] = total_rows(mate_sum[one])

            for part, (first, number) in enumerate(total_parts):

                @pl.when(unit == first + number - 1)
                def _():
                    back_total_copy(part).start()

            back_copy(group).start()

    @pl.loop(ready * pair, units + max(back_lag, own_lag))
    def _(i):
        @pl.when(jnp.logical_and(i < units, lax.rem(i, pair) == 0))
        def _():
            forward(i // pair)

        unit = i - lag

        @pl.when(jnp.logical_and(unit >= 0, unit < units))
        def _():
            h = head_of(unit)

            @pl.when(has_behind)
            def _():
                forward_copy(unit, mate).wait_recv()

            far = weighted(query_far[unit], keys[far_version, h], values[far_version, h])
            mate_sum[unit] = weighted(
                query_mate[unit], keys[mate_version, h], values[mate_version, h]
            )
            far_out[unit] = far[:, 0:head].astype(bf16)
            far_total_out[unit] = total_rows(far)

            @pl.when(has_behind)
            def _():
                far_copy(unit, behind).start()

                @pl.when(lax.rem(unit, pair) == pair - 1)
                def _():
                    far_total_copy(unit // pair, behind).start()

        @pl.when(jnp.logical_and(i >= back_lag, i < units + back_lag))
        def _():
            send_back(i - back_lag)

        own = i - own_lag

        @pl.when(own >= 0)
        def _():
            h = head_of(own)
            own_sum[own] = weighted(query[own], keys[0, h], values[0, h]) + weighted(
                query[own], text_keys[h], text_values[h]
            )

    def arrive(unit):
        back_copy(unit // pair).wait_recv()

    def gathered(unit):
        total = jnp.transpose(jnp.broadcast_to(back_total_in[unit], (head, rows)))
        mine = own_sum[unit]
        return (
            (mine[:, 0:head] + back_in[unit].astype(f32)) / (mine[:, head : 2 * head] + total)
        ).astype(bf16)

    def gather_range(half, first, last_unit, place):
        @pl.loop(0, (last_unit - first) // pair)
        def _(c):
            arrive(first + c * pair)
            for j in range(pair):
                lanes = pl.ds(pl.multiple_of((place + c * pair + j) * head, head), head)
                attended[half, :, lanes] = gathered(first + c * pair + j)

    mixed_copy = pltpu.make_async_remote_copy(
        src_ref=mixed_out,
        dst_ref=mixed_in,
        send_sem=send_sem.at[7],
        recv_sem=mixed_sem.at[0],
        device_id={"head": other_core},
        device_id_type=MESH,
    )
    full = output_weight.shape[1]
    wide = 512 if full % 512 == 0 else full

    for copy in output_loads:
        copy.wait()
    back_total_copy(0).wait_recv()
    gather_range(1, pair, pair + heads - pair, pair)
    gather_range(1, heads, pair + heads, 0)

    @pl.loop(0, full // wide)
    def _(c):
        here = pl.ds(pl.multiple_of(c * wide, wide), wide)
        mixed_out[:, here] = jnp.dot(
            attended[1], output_weight[:, here], preferred_element_type=f32
        ).astype(bf16)

    mixed_copy.start()
    gather_range(0, 0, pair, 0)
    for part in range(1, len(total_parts) - 1):
        first, number = total_parts[part]
        back_total_copy(part).wait_recv()
        gather_range(0, first, first + number, first - heads)
    most = width - span
    mixed_copy.wait_recv()

    @pl.loop(0, full // wide)
    def _(c):
        here = pl.ds(pl.multiple_of(c * wide, wide), wide)
        mixed = mixed_in[:, here].astype(f32) + jnp.dot(
            attended[0, :, 0:most], output_weight[0:most, here], preferred_element_type=f32
        )
        base[:, here] = tokens_ref[:, here].astype(f32) + modulation_ref[2:3, here] * mixed

    if len(total_parts) > 1:
        back_total_copy(len(total_parts) - 1).wait_recv()
    arrive(units - pair)
    for j in range(pair):
        last[:, j * head : (j + 1) * head] = gathered(units - pair + j)
    sent(normed.at[0], normed.at[1], 0, "head", other_core)
    mixed_copy.wait_send()
    sent(query, query_mate, 1, "section", mate)
    sent(back_out, back_in, 5, "section", mate)
    sent(back_total_out, back_total_in, 6, "section", mate)

    @pl.when(has_ahead)
    def _():
        sent(query_mate, query_far, 2, "section", mate)

    @pl.when(has_behind)
    def _():
        sent(far_out, far_in, 3, "section", mate)
        sent(far_total_out, far_total_in, 4, "section", mate)


def finish(base, last, last_weight, modulation, raw, updated_hbm, raw_hbm, updated, sems):
    full = base.shape[1]
    wide = 512 if full % 512 == 0 else full
    raw_copy = pltpu.make_async_copy(raw, raw_hbm, sems.at[0])
    raw_copy.start()
    for c in range(full // wide):
        here = slice(c * wide, (c + 1) * wide)
        updated[:, here] = (
            base[:, here]
            + modulation[2:3, here]
            * jnp.dot(last[...], last_weight[:, here], preferred_element_type=f32)
        ).astype(bf16)
        pltpu.make_async_copy(updated.at[:, here], updated_hbm.at[:, here], sems.at[1]).start()
    pltpu.make_async_copy(updated, updated_hbm, sems.at[1]).wait()
    raw_copy.wait()


def on_device(
    video_tokens,
    modulation,
    project_weight,
    output_weight,
    norm_gains,
    text_cache,
    text_count,
    video_keep,
    patch_order,
    stale_cache,
):
    head = norm_gains.shape[1]
    rows, model = video_tokens.shape
    width = project_weight.shape[2]
    patch = stale_cache.shape[1]
    text_rows = text_cache.shape[1]
    heads = width // head
    units = 2 * heads
    pair = 2 if heads % 2 == 0 else 1
    pairs = heads // pair
    vmem = pl.BlockSpec(memory_space=pltpu.VMEM)
    hbm = pl.BlockSpec(memory_space=pl.ANY)
    unit_rows = pltpu.VMEM((units, rows, head), bf16)
    unit_totals = pltpu.VMEM((units, 1, rows), f32)
    unit_sums = pltpu.VMEM((units, rows, 2 * head), f32)
    handed = pl.pallas_call(
        kernel,
        out_shape=(
            pltpu.VMEM(video_tokens.shape, f32),
            pltpu.VMEM((rows, pair * head), bf16),
            pltpu.VMEM((pair * head, model), bf16),
            pltpu.VMEM(modulation.shape, f32),
            pltpu.VMEM(stale_cache.shape, bf16),
        ),
        in_specs=[hbm, pl.BlockSpec(memory_space=pltpu.SMEM)] + [hbm] * 8,
        out_specs=(vmem,) * 5,
        scratch_shapes=[
            pltpu.SMEM(patch_order.shape, jnp.int32),
            pltpu.VMEM(video_tokens.shape, bf16),
            pltpu.VMEM(norm_gains.shape, f32),
            pltpu.VMEM(video_keep.shape, jnp.int32),
            pltpu.VMEM(project_weight.shape, bf16),
            pltpu.VMEM(output_weight.shape, bf16),
            pltpu.VMEM(text_cache.shape, bf16),
            pltpu.VMEM(stale_cache.shape, bf16),
            pltpu.VMEM((2, rows, model), bf16),
            unit_rows,
            unit_rows,
            unit_rows,
            pltpu.VMEM((2, heads, patch, head), bf16),
            pltpu.VMEM((2, heads, patch, 2 * head), bf16),
            pltpu.VMEM((heads, text_rows, head), bf16),
            pltpu.VMEM((heads, text_rows, 2 * head), bf16),
            unit_sums,
            unit_sums,
            unit_rows,
            unit_totals,
            unit_rows,
            unit_totals,
            unit_rows,
            unit_totals,
            unit_rows,
            unit_totals,
            pltpu.VMEM((2, rows, width), bf16),
            pltpu.VMEM((rows, model), bf16),
            pltpu.VMEM((rows, model), bf16),
            pltpu.SemaphoreType.DMA((14,)),
            pltpu.SemaphoreType.DMA((8,)),
            pltpu.SemaphoreType.DMA((2,)),
            pltpu.SemaphoreType.DMA((2 * pairs + 1,)),
            pltpu.SemaphoreType.DMA((units,)),
            pltpu.SemaphoreType.DMA((units,)),
            pltpu.SemaphoreType.DMA((2 * pairs,)),
            pltpu.SemaphoreType.DMA((2 * pairs,)),
            pltpu.SemaphoreType.DMA((pairs,)),
            pltpu.SemaphoreType.DMA((1,)),
            pltpu.SemaphoreType.REGULAR,
        ],
        compiler_params=pltpu.CompilerParams(
            collective_id=0, has_side_effects=True, vmem_limit_bytes=52 * 1024 * 1024
        ),
    )(
        patch_order,
        text_count,
        video_tokens,
        modulation,
        norm_gains,
        video_keep,
        project_weight,
        output_weight,
        text_cache,
        stale_cache,
    )
    return pl.pallas_call(
        finish,
        out_shape=(
            jax.ShapeDtypeStruct(video_tokens.shape, bf16),
            jax.ShapeDtypeStruct(stale_cache.shape, bf16),
        ),
        in_specs=[vmem] * 5,
        out_specs=(hbm, hbm),
        scratch_shapes=[
            pltpu.VMEM(video_tokens.shape, bf16),
            pltpu.SemaphoreType.DMA((2,)),
        ],
        compiler_params=pltpu.CompilerParams(vmem_limit_bytes=16 * 1024 * 1024),
    )(*[pltpu.with_memory_space_constraint(array, pltpu.VMEM) for array in handed])


def solution(mesh):
    placed = (
        P(("groups", "section", "head"), None),
        P("groups", None),
        P(None, None, "head"),
        P("head", None),
        P(),
        P(None, "groups", "head"),
        P("groups"),
        P("groups"),
        P("groups"),
        P(None, ("groups", "section"), "head"),
    )
    return jax.shard_map(
        on_device,
        mesh=mesh,
        in_specs=placed,
        out_specs=(P(("groups", "section", "head"), None), P(None, ("groups", "section"), "head")),
        check_vma=False,
    )
```
